32 devices in a mesh: dp: 8 (over y, x, core), expert: 4 (over z).
Axes of the slice: x: 2, y: 2, z: 4, core: 2. Of those that a mesh axis runs over, the one named last changes fastest.
Arguments:
- tokens: bfloat16 [4096, 2048], P(('dp', 'expert')), may hold values from -6 to 6
- out_grad: bfloat16 [4096, 2048], P(('dp', 'expert')), may hold values from -6 to 6
- gate_prob: float32 [4096, 1], P(('dp', 'expert')), may hold values from 0.2 to 1
- routing: int32 [4096, 1], P(('dp', 'expert')), may hold values from 0 to 3; in each aligned block of 128 rows (0 to 127, 128 to 255, ...) at most 64 rows name the same one
- expert_weights: bfloat16 [4, 2048, 1152], P('expert'), may hold values from -0.125 to 0.125
Outputs:
- input_grad: bfloat16 [4096, 2048], P(('dp', 'expert'))
- weight_grad: float32 [4, 2048, 1152], P('expert', 'dp')
The draws below stay inside these ranges and needn't reach their ends.
Inputs may be any that keep to these rules, and one draw needn't show every extreme that they name: `routing`: among the tokens of one device at most 64 go to any one expert; in some devices' tokens an expert gets exactly 64.
All inputs are finite; a program needn't handle non-finite values.
Results may differ from the reference program's by a relative error of at most 0.014.
Values may be sent and summed in bfloat16 or wider, within the bound.
A program may use at most 64 MiB of HBM per device.

```python
import math
from functools import partial
import jax
import jax.numpy as jnp
import numpy as np
from jax import lax

D = 2048
FF = 384
TOK_DEV = 128
TOKENS = 4096
EXPERTS_TURN = 4
CAP = 64
GROUP_ROWS = 1024
N_DP = 8
N_EXPERT = 4


def block_levels(key, shape, shards, smallest, high):
    level, own = 1.0, jax.random.fold_in(key, 6)
    for axis_at, shards_of in shards:
        heights = jnp.exp(jax.random.uniform(jax.random.fold_in(own, axis_at), (shards_of,), jnp.float32, smallest / len(shards), high / len(shards)))
        level = level * jnp.repeat(heights, shape[axis_at] // shards_of).reshape([-1 if axis == axis_at else 1 for axis in range(len(shape))])
    return level


def shared_out(stream_key, own, number, rows, number_of, top, most, slope):
    order = jax.random.permutation(stream_key, number_of)
    heavy_load, common = shares(number_of, rows * top, most, slope, True), shares(number_of, rows * top, most, slope, False)
    places = jnp.arange(number_of)

    def named(sizes, rotation):
        used = int((sizes > 0).sum())
        fixed = max(1, used // 4)
        moved = fixed + (places - fixed + rotation * (used - fixed)) % max(1, number_of - fixed)
        return jnp.zeros((number_of,), jnp.int32).at[order[jnp.where(places < fixed, places, moved)]].set(jnp.asarray(sizes, jnp.int32))

    sizes = jnp.where(number % 4 == 0, named(heavy_load, number // 4), named(common, number - number // 4 - 1))
    mixed = jax.random.permutation(jax.random.fold_in(own, 3), number_of)
    giver, receiver = mixed[0:number_of // 2 * 2:2], mixed[1:number_of // 2 * 2:2]
    slack = jnp.minimum(sizes[giver] - 1, most - sizes[receiver]) // 2
    slack = jnp.where((giver == order[0]) | (receiver == order[0]) | (sizes[receiver] == 0), 0, jnp.maximum(slack, 0))
    moved = jax.random.randint(jax.random.fold_in(own, 4), (number_of // 2,), 0, 1 << 20) % (slack + 1)
    sizes = sizes.at[giver].add(-moved).at[receiver].add(moved)
    labels = jnp.searchsorted(jnp.cumsum(sizes), jnp.arange(rows * top), side="right").astype(jnp.int32)
    grid = labels.reshape(top, rows).T
    grid = grid[jax.random.permutation(jax.random.fold_in(own, 1), rows)]
    rotation = jax.random.randint(jax.random.fold_in(own, 2), (rows, 1), 0, top)
    return jnp.take_along_axis(grid, (jnp.arange(top)[None, :] + rotation) % top, axis=1)


def shares(number_of, total, reach, slope, full):
    loads = [(1 << 20) // math.isqrt(standing ** slope) + 1 for standing in range(1, number_of + 1)]
    largest = reach if full else min(reach, max(-(-total // number_of), total * loads[0] // sum(loads)))
    least = 1 if total - largest >= number_of - 1 else 0
    counts, rest = [largest] + [least] * (number_of - 1), total - largest - least * (number_of - 1)
    while rest > 0:
        candidates = [i for i in range(1, number_of) if counts[i] < largest] or [i for i in range(1, number_of) if counts[i] < reach]
        whole, left = sum([loads[i] for i in candidates]), rest
        for i in candidates:
            more = min(reach - counts[i], max(1, left * loads[i] // whole), rest)
            counts[i] = counts[i] + more
            rest = rest - more
    return np.array(counts)


def noise(rng, extent, width, reach, pieces=(), kind=jnp.bfloat16):
    drawn = jax.random.normal(rng, extent, jnp.float32) * width
    if len(pieces) > 0:
        drawn = block_levels(rng, extent, pieces, -0.22, 0.18) * drawn
    return jnp.clip(drawn, min=-reach, max=reach).astype(kind)


def setup_inputs(seed: int = 0) -> dict:
    streams_of = jax.random.split(jax.random.key(seed), 6)
    tokens = noise(streams_of[0], (TOKENS, D), 1.0, 6.0, ((0, 32),))
    out_grad = noise(streams_of[1], (TOKENS, D), 1.0, 6.0, ((0, 32),))
    gate_prob = jnp.clip(0.2 + 0.8 * jax.random.uniform(streams_of[2], (TOKENS, 1), jnp.float32) ** block_levels(streams_of[2], (TOKENS, 1), ((0, 32),), -0.2, 0.2), 0.2, 1.0)
    routing_keys = jax.random.split(jax.random.fold_in(streams_of[3], 1), TOKENS // TOK_DEV)
    routing_turns = jax.random.permutation(jax.random.fold_in(streams_of[3], 3), TOKENS // TOK_DEV)
    routing = jax.vmap(lambda own, number: shared_out(jax.random.fold_in(streams_of[3], 2), own, number, TOK_DEV, N_EXPERT, 1, CAP, 2))(routing_keys, routing_turns).reshape((TOKENS, 1))
    expert_weights = noise(streams_of[4], (EXPERTS_TURN, D, 3 * FF), D ** -0.5, 0.125, ((0, 4),))
    return {"tokens": tokens, "out_grad": out_grad, "gate_prob": gate_prob, "routing": routing, "expert_weights": expert_weights}


def slot_of(route_block, capacity, experts):
    onehot = (route_block[:, None] == jnp.arange(experts, dtype=jnp.int32)[None, :]).astype(jnp.int32)
    before = jnp.cumsum(onehot, axis=0) - onehot
    position = jnp.sum(before * onehot, axis=1).astype(jnp.int32)
    return (route_block * capacity + position).astype(jnp.int32)


def expert_rows(weights, rows_in, grad_in):
    hidden_width = weights.shape[1] // 3
    pair_weights = weights[:, :2 * hidden_width]
    down_weights = weights[:, 2 * hidden_width:]
    pre_act = jnp.dot(rows_in, pair_weights, preferred_element_type=jnp.float32)
    pre_gate = pre_act[:, :hidden_width]
    pre_up = pre_act[:, hidden_width:]
    sigmoid_gate = jax.nn.sigmoid(pre_gate)
    active = pre_gate * sigmoid_gate
    hidden = (active * pre_up).astype(jnp.bfloat16)
    grad_hidden = jnp.dot(grad_in, down_weights, preferred_element_type=jnp.float32)
    grad_gate = grad_hidden * pre_up * (sigmoid_gate * (1.0 + pre_gate * (1.0 - sigmoid_gate)))
    grad_up = grad_hidden * active
    grad_pair = jnp.concatenate([grad_gate.astype(jnp.bfloat16), grad_up.astype(jnp.bfloat16)], axis=1)
    returned = lax.dot_general(grad_pair, pair_weights, (((1,), (1,)), ((), ())), preferred_element_type=jnp.float32)
    return returned.astype(jnp.bfloat16), hidden, grad_pair


def weight_term(rows_in, grad_in, hidden, grad_pair, grad_scale):
    contract = (((0,), (0,)), ((), ()))
    first_part = lax.dot_general(rows_in, grad_pair, contract, preferred_element_type=jnp.float32)
    second = lax.dot_general(grad_in, hidden, contract, preferred_element_type=jnp.float32)
    return grad_scale * jnp.concatenate([first_part, second], axis=1)


def reference(tokens, out_grad, gate_prob, routing, expert_weights):
    model_width = tokens.shape[1]
    grad_scale = float(GROUP_ROWS) ** -0.5
    scaled = (gate_prob * out_grad.astype(jnp.float32)).astype(jnp.bfloat16)
    tok_x = tokens.reshape(N_DP, N_EXPERT, TOK_DEV, model_width)
    tok_g = scaled.reshape(N_DP, N_EXPERT, TOK_DEV, model_width)
    routes = routing.reshape(N_DP, N_EXPERT, TOK_DEV)
    slotter = jax.vmap(partial(slot_of, capacity=CAP, experts=N_EXPERT))

    def one_expert(operands):
        weights, rows_in, grad_in = operands
        returned, hidden, grad_pair = expert_rows(weights, rows_in, grad_in)
        rounded = weight_term(rows_in, grad_in, hidden, grad_pair, grad_scale).astype(jnp.bfloat16)
        rounded = lax.optimization_barrier(rounded)
        return returned, rounded.astype(jnp.float32)

    def replica(running, blocks):
        block_x, block_g, block_r = blocks
        slot_index = slotter(block_r)
        source = jnp.broadcast_to(jnp.arange(N_EXPERT, dtype=jnp.int32)[:, None], slot_index.shape)
        buf_x = jnp.zeros((N_EXPERT, N_EXPERT * CAP, model_width), jnp.bfloat16).at[source, slot_index].set(block_x)
        buf_g = jnp.zeros((N_EXPERT, N_EXPERT * CAP, model_width), jnp.bfloat16).at[source, slot_index].set(block_g)
        buf_x = buf_x.reshape(N_EXPERT, N_EXPERT, CAP, model_width).transpose(1, 0, 2, 3).reshape(N_EXPERT, N_EXPERT * CAP, model_width)
        buf_g = buf_g.reshape(N_EXPERT, N_EXPERT, CAP, model_width).transpose(1, 0, 2, 3).reshape(N_EXPERT, N_EXPERT * CAP, model_width)
        returned, terms = lax.map(one_expert, (expert_weights, buf_x, buf_g))
        returned = returned.reshape(N_EXPERT, N_EXPERT, CAP, model_width).transpose(1, 0, 2, 3).reshape(N_EXPERT, N_EXPERT * CAP, model_width)
        return running + terms, returned[source, slot_index]

    initial = jnp.zeros((N_EXPERT, model_width, expert_weights.shape[2]), jnp.float32)
    totals, input_grads = lax.scan(replica, initial, (tok_x, tok_g, routes))
    return input_grads.reshape(TOKENS, model_width), totals
```

```python
import functools
import math
import jax
import jax.numpy as jnp
from jax import lax
from jax.experimental import pallas as pl
from jax.experimental.pallas import tpu as pltpu
from jax.sharding import PartitionSpec as P

MESH = pl.DeviceIdType.MESH
F32 = jnp.float32
BF16 = jnp.bfloat16


def xor(value, step):
    total, bit = 0, 1
    result = value
    while bit <= step:
        if step & bit:
            result = result + bit - 2 * bit * (lax.rem(lax.div(value, bit), 2))
        bit *= 2
    return result


def plan(n_expert, n_dp):
    half = n_expert // 2
    near = list(range(1, half))
    far = list(range(n_expert - 1, half - 1, -1))
    chips = n_dp // 2
    side = math.isqrt(chips)
    while chips % side:
        side -= 1
    return near, far, chips // side, side


def body(
    n_expert,
    n_dp,
    cap,
    tokens_ref,
    out_grad_ref,
    gate_ref,
    route_col_ref,
    route_row_ref,
    w_hbm,
    in_grad_ref,
    w_grad_ref,
    w_ref,
    send_x,
    send_g,
    recv_x,
    recv_g,
    ret,
    arrived,
    pair,
    hidden,
    part,
    recv_a,
    send_b,
    recv_b,
    send_c,
    recv_c,
    w_sem,
    dx_s,
    dx_r,
    dg_s,
    dg_r,
    rt_s,
    rt_r,
    a_s,
    a_r,
    b_s,
    b_r,
    c_s,
    c_r,
):
    near, far, na, nb = plan(n_expert, n_dp)
    me = lax.axis_index("expert")
    dp = lax.axis_index("dp")
    tok, width = tokens_ref.shape
    hid = w_ref.shape[1] // 3
    slots = n_expert * cap
    half_rows = slots // 2
    share = width // n_dp
    grad_scale = float(tok * n_dp) ** (-0.5)
    core = lax.rem(dp, 2)
    chip = lax.div(dp, 2)
    pos_hi, pos_lo = lax.div(chip, na), lax.rem(chip, na)
    if na == nb:
        a = jnp.where(core == 0, pos_lo, pos_hi)
        b = jnp.where(core == 0, pos_hi, pos_lo)
    else:
        a, b = pos_lo, pos_hi

    def chip_of(a_at, b_at):
        plain = b_at * na + a_at
        if na == nb:
            return jnp.where(core == 0, plain, a_at * na + b_at)
        return plain

    def dp_of(a_at, b_at):
        return chip_of(a_at, b_at) * 2 + core

    w_copy = pltpu.make_async_copy(w_hbm.at[0], w_ref, w_sem)
    w_copy.start()

    barrier = pltpu.get_barrier_semaphore()
    partner = dp + 1 - 2 * core
    greeted = 0
    for k in near + far:
        pl.semaphore_signal(barrier, inc=1, device_id={"expert": xor(me, k)}, device_id_type=MESH)
        greeted += 1
    pl.semaphore_signal(barrier, inc=1, device_id={"dp": partner}, device_id_type=MESH)
    greeted += 1
    for s in range(1, na):
        pl.semaphore_signal(
            barrier, inc=1, device_id={"dp": dp_of(lax.rem(a + s, na), b)}, device_id_type=MESH
        )
        greeted += 1
    for t in range(1, nb):
        pl.semaphore_signal(
            barrier, inc=1, device_id={"dp": dp_of(a, lax.rem(b + t, nb))}, device_id_type=MESH
        )
        greeted += 1

    route_row = route_row_ref[...]
    route_col = route_col_ref[...]
    row_i = lax.broadcasted_iota(jnp.int32, (tok, tok), 0)
    col_i = lax.broadcasted_iota(jnp.int32, (tok, tok), 1)
    same = route_col == route_row
    pos_row = jnp.sum(jnp.where(same & (row_i < col_i), 1.0, 0.0), axis=0, keepdims=True)
    pos_col = jnp.sum(jnp.where(same & (col_i < row_i), 1.0, 0.0), axis=1, keepdims=True)
    slot_row = route_row.astype(F32) * cap + pos_row
    slot_col = route_col.astype(F32) * cap + pos_col
    slot_at = lax.broadcasted_iota(jnp.int32, (slots, tok), 0).astype(F32)
    table = jnp.where(slot_at == slot_row, 1.0, 0.0).astype(BF16)
    slot_of = lax.broadcasted_iota(jnp.int32, (tok, slots), 1).astype(F32)
    table_t = jnp.where(slot_of == slot_col, 1.0, 0.0).astype(BF16)

    send_x[...] = jnp.dot(table, tokens_ref[...], preferred_element_type=F32).astype(BF16)
    scaled = (gate_ref[...] * out_grad_ref[...].astype(F32)).astype(BF16)
    send_g[...] = jnp.dot(table, scaled, preferred_element_type=F32).astype(BF16)

    def rows_of(index):
        return pl.ds(pl.multiple_of(index * cap, cap), cap)

    pl.semaphore_wait(barrier, greeted)

    def dispatch(k, src, dst, s_sem, r_sem):
        peer = xor(me, k)
        return pltpu.make_async_remote_copy(
            src_ref=src.at[rows_of(peer)],
            dst_ref=dst.at[rows_of(me)],
            send_sem=s_sem.at[k],
            recv_sem=r_sem.at[k],
            device_id={"expert": peer},
            device_id_type=MESH,
        )

    x_copies = {k: dispatch(k, send_x, recv_x, dx_s, dx_r) for k in near + far}
    g_copies = {k: dispatch(k, send_g, recv_g, dg_s, dg_r) for k in near + far}
    returns = {k: dispatch(k, ret, arrived, rt_s, rt_r) for k in near + far}
    for k in near + far:
        x_copies[k].start()
        g_copies[k].start()

    recv_x[rows_of(me)] = send_x[rows_of(me)]
    recv_g[rows_of(me)] = send_g[rows_of(me)]
    w_copy.wait()

    mine = lax.div(me, n_expert // 2) if n_expert > 1 else 0

    def forward(start):
        rows = pl.ds(pl.multiple_of(start, cap), half_rows)
        x = recv_x[rows]
        pre_gate = jnp.dot(x, w_ref[:, :hid], preferred_element_type=F32)
        pre_up = jnp.dot(x, w_ref[:, hid : 2 * hid], preferred_element_type=F32)
        grad_hidden = jnp.dot(recv_g[rows], w_ref[:, 2 * hid :], preferred_element_type=F32)
        sig = jax.nn.sigmoid(pre_gate)
        active = pre_gate * sig
        hidden[rows] = (active * pre_up).astype(BF16)
        grad_gate = grad_hidden * pre_up * (sig * (1.0 + pre_gate * (1.0 - sig)))
        pair[rows, :hid] = grad_gate.astype(BF16)
        pair[rows, hid:] = (grad_hidden * active).astype(BF16)

    def backward(start):
        rows = pl.ds(pl.multiple_of(start, cap), half_rows)
        tile = min(512, width)

        @pl.loop(0, width // tile)
        def _(j):
            at = pl.ds(pl.multiple_of(j * tile, tile), tile)
            ret[rows, at] = lax.dot_general(
                pair[rows],
                w_ref[at, : 2 * hid],
                (((1,), (1,)), ((), ())),
                preferred_element_type=F32,
            ).astype(BF16)

    first_half = mine * half_rows
    other_half = (1 - mine) * half_rows
    for k in near:
        x_copies[k].wait_recv()
        g_copies[k].wait_recv()
    forward(first_half)
    backward(first_half)
    for k in near:
        returns[k].start()
    arrived[rows_of(me)] = ret[rows_of(me)]
    for k in far:
        x_copies[k].wait_recv()
        g_copies[k].wait_recv()
    forward(other_half)
    backward(other_half)
    for k in far:
        returns[k].start()

    def weight_rows(start, size):
        at = pl.ds(pl.multiple_of(start, size), size)
        contract = (((0,), (0,)), ((), ()))
        part[at, : 2 * hid] = (
            grad_scale
            * lax.dot_general(recv_x[:, at], pair[...], contract, preferred_element_type=F32)
        ).astype(BF16)
        part[at, 2 * hid :] = (
            grad_scale
            * lax.dot_general(recv_g[:, at], hidden[...], contract, preferred_element_type=F32)
        ).astype(BF16)

    def band(chip_at, core_at):
        return pl.ds(pl.multiple_of((chip_at * 2 + core_at) * share, share), share)

    items = [(s, t) for s in range(1, na) for t in list(range(1, nb)) + [0]]
    items += [(0, t) for t in list(range(1, nb)) + [0]]

    def item_chip(s, t):
        return chip_of(lax.rem(a + s, na), lax.rem(b + t, nb))

    banded = share % 128 == 0
    if not banded:

        @pl.loop(0, width // 256)
        def _(j):
            weight_rows(j * 256, 256)

    def pair_copy(index, chip_at):
        rows = band(chip_at, 1 - core)
        return pltpu.make_async_remote_copy(
            src_ref=part.at[rows],
            dst_ref=recv_a.at[pl.ds(pl.multiple_of(chip_at * share, share), share)],
            send_sem=a_s.at[index],
            recv_sem=a_r.at[index],
            device_id={"dp": partner},
            device_id_type=MESH,
        )

    def partner_chip(s, t):
        if na == nb:
            a_at, b_at = lax.rem(b + s, na), lax.rem(a + t, nb)
            return jnp.where(core == 1, b_at * na + a_at, a_at * na + b_at)
        return item_chip(s, t)

    a_copies = []
    for index, (s, t) in enumerate(items):
        chip_at = partner_chip(s, t)
        if banded:
            weight_rows((chip_at * 2 + 1 - core) * share, share)
        copy = pair_copy(index, chip_at)
        copy.start()
        a_copies.append(copy)

    def pair_sum(index, s, t):
        chip_at = item_chip(s, t)
        a_copies[index].wait_recv()
        return (
            part[band(chip_at, core)].astype(F32)
            + recv_a[pl.ds(pl.multiple_of(chip_at * share, share), share)].astype(F32)
        )

    if banded:
        for s, t in items:
            weight_rows((item_chip(s, t) * 2 + core) * share, share)

    b_copies = {}
    for index, (s, t) in enumerate(items):
        if s == 0:
            continue
        at = (s - 1) * nb + t
        send_b[at] = pair_sum(index, s, t).astype(BF16)
        copy = pltpu.make_async_remote_copy(
            src_ref=send_b.at[at],
            dst_ref=recv_b.at[at],
            send_sem=b_s.at[at],
            recv_sem=b_r.at[at],
            device_id={"dp": dp_of(lax.rem(a + s, na), b)},
            device_id_type=MESH,
        )
        copy.start()
        b_copies[s, t] = copy
    c_copies = {}
    for index, (s, t) in enumerate(items):
        if s > 0:
            continue
        total = pair_sum(index, s, t)
        for s_from in range(1, na):
            b_copies[s_from, t].wait_recv()
            total = total + recv_b[(s_from - 1) * nb + t].astype(F32)
        if t > 0:
            send_c[t - 1] = total.astype(BF16)
            copy = pltpu.make_async_remote_copy(
                src_ref=send_c.at[t - 1],
                dst_ref=recv_c.at[t - 1],
                send_sem=c_s.at[t - 1],
                recv_sem=c_r.at[t - 1],
                device_id={"dp": dp_of(a, lax.rem(b + t, nb))},
                device_id_type=MESH,
            )
            copy.start()
            c_copies[t] = copy
        else:
            w_grad_ref[0] = total
    for t in range(1, nb):
        c_copies[t].wait_recv()
        w_grad_ref[0] += recv_c[t - 1].astype(F32)

    for k in near + far:
        returns[k].wait_recv()
    in_grad_ref[...] = jnp.dot(table_t, arrived[...], preferred_element_type=F32).astype(BF16)

    for k in near + far:
        x_copies[k].wait_send()
        g_copies[k].wait_send()
        returns[k].wait_send()
    for copy in a_copies + list(b_copies.values()) + list(c_copies.values()):
        copy.wait_send()


def local(n_expert, n_dp, tokens, out_grad, gate_prob, routing, expert_weights):
    tok, width = tokens.shape
    full = expert_weights.shape[2]
    hid = full // 3
    cap = max(16, 2 * tok // n_expert)
    slots = n_expert * cap
    share = width // n_dp
    _, _, na, nb = plan(n_expert, n_dp)
    chips = na * nb
    n_b, n_c = max(1, (na - 1) * nb), max(1, nb - 1)
    dma = pltpu.SemaphoreType.DMA
    vmem = pl.BlockSpec(memory_space=pltpu.VMEM)
    return pl.pallas_call(
        functools.partial(body, n_expert, n_dp, cap),
        out_shape=(
            jax.ShapeDtypeStruct((tok, width), BF16),
            jax.ShapeDtypeStruct((1, share, full), F32),
        ),
        in_specs=[vmem] * 5 + [pl.BlockSpec(memory_space=pl.ANY)],
        out_specs=(vmem, vmem),
        scratch_shapes=[
            pltpu.VMEM((width, full), BF16),
            pltpu.VMEM((slots, width), BF16),
            pltpu.VMEM((slots, width), BF16),
            pltpu.VMEM((slots, width), BF16),
            pltpu.VMEM((slots, width), BF16),
            pltpu.VMEM((slots, width), BF16),
            pltpu.VMEM((slots, width), BF16),
            pltpu.VMEM((slots, 2 * hid), BF16),
            pltpu.VMEM((slots, hid), BF16),
            pltpu.VMEM((width, full), BF16),
            pltpu.VMEM((chips * share, full), BF16),
            pltpu.VMEM((n_b, share, full), BF16),
            pltpu.VMEM((n_b, share, full), BF16),
            pltpu.VMEM((n_c, share, full), BF16),
            pltpu.VMEM((n_c, share, full), BF16),
            dma,
            dma((n_expert,)),
            dma((n_expert,)),
            dma((n_expert,)),
            dma((n_expert,)),
            dma((n_expert,)),
            dma((n_expert,)),
            dma((chips,)),
            dma((chips,)),
            dma((n_b,)),
            dma((n_b,)),
            dma((n_c,)),
            dma((n_c,)),
        ],
        compiler_params=pltpu.CompilerParams(
            collective_id=0, has_side_effects=True, vmem_limit_bytes=60 * 1024 * 1024
        ),
        name="moe_backward",
    )(tokens, out_grad, gate_prob, routing, routing.reshape(1, tok), expert_weights)


def solution(mesh):
    tokens_spec = P(("dp", "expert"), None)
    return jax.shard_map(
        functools.partial(local, mesh.shape["expert"], mesh.shape["dp"]),
        mesh=mesh,
        in_specs=(tokens_spec, tokens_spec, tokens_spec, tokens_spec, P("expert", None, None)),
        out_specs=(tokens_spec, P("expert", "dp", None)),
        check_vma=False,
    )
```

```python
import functools
import math
import jax
import jax.numpy as jnp
from jax import lax
from jax.experimental import pallas as pl
from jax.experimental.pallas import tpu as pltpu
from jax.sharding import PartitionSpec as P

MESH = pl.DeviceIdType.MESH
F32 = jnp.float32
BF16 = jnp.bfloat16
SUBS = 2


def xor(value, step):
    total, bit = 0, 1
    result = value
    while bit <= step:
        if step & bit:
            result = result + bit - 2 * bit * (lax.rem(lax.div(value, bit), 2))
        bit *= 2
    return result


def plan(n_expert, n_dp):
    half, quarter = n_expert // 2, n_expert // 4
    near = list(range(1, half))
    across = list(range(n_expert - 1, half + quarter - 1, -1))
    last = list(range(half + quarter - 1, half - 1, -1))
    chips = n_dp // 2
    side = math.isqrt(chips)
    while chips % side:
        side -= 1
    return near, across, last, chips // side, side


def body(
    n_expert,
    n_dp,
    cap,
    tokens_ref,
    out_grad_ref,
    gate_ref,
    route_col_ref,
    route_row_ref,
    w_hbm,
    in_grad_ref,
    w_grad_ref,
    w_ref,
    send_x,
    send_g,
    recv_x,
    recv_g,
    ret,
    arrived,
    pair,
    hidden,
    part,
    recv_a,
    send_b,
    recv_b,
    send_c,
    recv_c,
    w_sem,
    dx_s,
    dx_r,
    dg_s,
    dg_r,
    rt_s,
    rt_r,
    a_s,
    a_r,
    b_s,
    b_r,
    c_s,
    c_r,
):
    near, across, last, na, nb = plan(n_expert, n_dp)
    far = across + last
    me = lax.axis_index("expert")
    dp = lax.axis_index("dp")
    tok, width = tokens_ref.shape
    hid = w_ref.shape[1] // 3
    slots = n_expert * cap
    quarter_rows = slots // 4
    share = width // n_dp
    sub = share // SUBS
    grad_scale = float(tok * n_dp) ** (-0.5)
    core = lax.rem(dp, 2)
    chip = lax.div(dp, 2)
    pos_hi, pos_lo = lax.div(chip, na), lax.rem(chip, na)
    if na == nb:
        a = jnp.where(core == 0, pos_lo, pos_hi)
        b = jnp.where(core == 0, pos_hi, pos_lo)
    else:
        a, b = pos_lo, pos_hi

    def chip_of(a_at, b_at):
        plain = b_at * na + a_at
        if na == nb:
            return jnp.where(core == 0, plain, a_at * na + b_at)
        return plain

    def dp_of(a_at, b_at):
        return chip_of(a_at, b_at) * 2 + core

    w_copy = pltpu.make_async_copy(w_hbm.at[0], w_ref, w_sem)
    w_copy.start()

    barrier = pltpu.get_barrier_semaphore()
    partner = dp + 1 - 2 * core
    greeted = 0
    for k in near + far:
        pl.semaphore_signal(barrier, inc=1, device_id={"expert": xor(me, k)}, device_id_type=MESH)
        greeted += 1
    pl.semaphore_signal(barrier, inc=1, device_id={"dp": partner}, device_id_type=MESH)
    greeted += 1
    for s in range(1, na):
        pl.semaphore_signal(
            barrier, inc=1, device_id={"dp": dp_of(lax.rem(a + s, na), b)}, device_id_type=MESH
        )
        greeted += 1
    for t in range(1, nb):
        pl.semaphore_signal(
            barrier, inc=1, device_id={"dp": dp_of(a, lax.rem(b + t, nb))}, device_id_type=MESH
        )
        greeted += 1

    route_row = route_row_ref[...]
    route_col = route_col_ref[...]
    row_i = lax.broadcasted_iota(jnp.int32, (tok, tok), 0)
    col_i = lax.broadcasted_iota(jnp.int32, (tok, tok), 1)
    same = route_col == route_row
    pos_row = jnp.sum(jnp.where(same & (row_i < col_i), 1.0, 0.0), axis=0, keepdims=True)
    pos_col = jnp.sum(jnp.where(same & (col_i < row_i), 1.0, 0.0), axis=1, keepdims=True)
    slot_row = route_row.astype(F32) * cap + pos_row
    slot_col = route_col.astype(F32) * cap + pos_col
    slot_at = lax.broadcasted_iota(jnp.int32, (slots, tok), 0).astype(F32)
    table = jnp.where(slot_at == slot_row, 1.0, 0.0).astype(BF16)
    slot_of = lax.broadcasted_iota(jnp.int32, (tok, slots), 1).astype(F32)
    table_t = jnp.where(slot_of == slot_col, 1.0, 0.0).astype(BF16)

    send_x[...] = jnp.dot(table, tokens_ref[...], preferred_element_type=F32).astype(BF16)
    scaled = (gate_ref[...] * out_grad_ref[...].astype(F32)).astype(BF16)
    send_g[...] = jnp.dot(table, scaled, preferred_element_type=F32).astype(BF16)

    def rows_of(index):
        return pl.ds(pl.multiple_of(index * cap, cap), cap)

    pl.semaphore_wait(barrier, greeted)

    def dispatch(k, src, dst, s_sem, r_sem):
        peer = xor(me, k)
        return pltpu.make_async_remote_copy(
            src_ref=src.at[rows_of(peer)],
            dst_ref=dst.at[rows_of(me)],
            send_sem=s_sem.at[k],
            recv_sem=r_sem.at[k],
            device_id={"expert": peer},
            device_id_type=MESH,
        )

    x_copies = {k: dispatch(k, send_x, recv_x, dx_s, dx_r) for k in near + far}
    g_copies = {k: dispatch(k, send_g, recv_g, dg_s, dg_r) for k in near + far}
    returns = {k: dispatch(k, ret, arrived, rt_s, rt_r) for k in near + far}
    for k in near + far:
        x_copies[k].start()
        g_copies[k].start()

    recv_x[rows_of(me)] = send_x[rows_of(me)]
    recv_g[rows_of(me)] = send_g[rows_of(me)]
    w_copy.wait()

    mine = lax.div(me, n_expert // 4)

    def forward(start, size):
        rows = pl.ds(pl.multiple_of(start, cap), size)
        x = recv_x[rows]
        pre_gate = jnp.dot(x, w_ref[:, :hid], preferred_element_type=F32)
        pre_up = jnp.dot(x, w_ref[:, hid : 2 * hid], preferred_element_type=F32)
        grad_hidden = jnp.dot(recv_g[rows], w_ref[:, 2 * hid :], preferred_element_type=F32)
        sig = jax.nn.sigmoid(pre_gate)
        active = pre_gate * sig
        hidden[rows] = (active * pre_up).astype(BF16)
        grad_gate = grad_hidden * pre_up * (sig * (1.0 + pre_gate * (1.0 - sig)))
        pair[rows, :hid] = grad_gate.astype(BF16)
        pair[rows, hid:] = (grad_hidden * active).astype(BF16)

    def backward(start, size):
        rows = pl.ds(pl.multiple_of(start, cap), size)
        tile = min(512, width)

        @pl.loop(0, width // tile)
        def _(j):
            at = pl.ds(pl.multiple_of(j * tile, tile), tile)
            ret[rows, at] = lax.dot_general(
                pair[rows],
                w_ref[at, : 2 * hid],
                (((1,), (1,)), ((), ())),
                preferred_element_type=F32,
            ).astype(BF16)

    near_half = (lax.div(mine, 2) * 2 * quarter_rows, 2 * quarter_rows)
    across_quarter = (xor(mine, 3) * quarter_rows, quarter_rows)
    last_quarter = (xor(mine, 2) * quarter_rows, quarter_rows)
    for k in near:
        x_copies[k].wait_recv()
        g_copies[k].wait_recv()
    forward(*near_half)
    backward(*near_half)
    for k in near:
        returns[k].start()
    arrived[rows_of(me)] = ret[rows_of(me)]
    for k in across:
        x_copies[k].wait_recv()
        g_copies[k].wait_recv()
    forward(*across_quarter)
    backward(*across_quarter)
    for k in last:
        x_copies[k].wait_recv()
        g_copies[k].wait_recv()
    for k in across:
        returns[k].start()
    forward(*last_quarter)

    def weight_rows(start, size):
        at = pl.ds(pl.multiple_of(start, size), size)
        contract = (((0,), (0,)), ((), ()))
        part[at, : 2 * hid] = (
            grad_scale
            * lax.dot_general(recv_x[:, at], pair[...], contract, preferred_element_type=F32)
        ).astype(BF16)
        part[at, 2 * hid :] = (
            grad_scale
            * lax.dot_general(recv_g[:, at], hidden[...], contract, preferred_element_type=F32)
        ).astype(BF16)

    def band(chip_at, core_at, g):
        return pl.ds(pl.multiple_of((chip_at * 2 + core_at) * share + g * sub, sub), sub)

    bands = [(s, t) for s in range(1, na) for t in list(range(1, nb)) + [0]]
    bands += [(0, t) for t in list(range(1, nb)) + [0]]
    items = [(s, t, g) for s, t in bands for g in range(SUBS)]

    def item_chip(s, t):
        return chip_of(lax.rem(a + s, na), lax.rem(b + t, nb))

    banded = share % 128 == 0
    if not banded:

        @pl.loop(0, width // 256)
        def _(j):
            weight_rows(j * 256, 256)

    def pair_copy(index, chip_at, g):
        rows = band(chip_at, 1 - core, g)
        return pltpu.make_async_remote_copy(
            src_ref=part.at[rows],
            dst_ref=recv_a.at[pl.ds(pl.multiple_of(chip_at * share + g * sub, sub), sub)],
            send_sem=a_s.at[index],
            recv_sem=a_r.at[index],
            device_id={"dp": partner},
            device_id_type=MESH,
        )

    def partner_chip(s, t):
        if na == nb:
            a_at, b_at = lax.rem(b + s, na), lax.rem(a + t, nb)
            return jnp.where(core == 1, b_at * na + a_at, a_at * na + b_at)
        return item_chip(s, t)

    a_copies = []
    for index, (s, t, g) in enumerate(items):
        chip_at = partner_chip(s, t)
        if banded and g == 0:
            weight_rows((chip_at * 2 + 1 - core) * share, share)
        copy = pair_copy(index, chip_at, g)
        copy.start()
        a_copies.append(copy)

    backward(*last_quarter)
    for k in last:
        returns[k].start()

    def pair_sum(index, s, t, g):
        chip_at = item_chip(s, t)
        a_copies[index].wait_recv()
        return (
            part[band(chip_at, core, g)].astype(F32)
            + recv_a[pl.ds(pl.multiple_of(chip_at * share + g * sub, sub), sub)].astype(F32)
        )

    if banded:
        for s, t in bands:
            weight_rows((item_chip(s, t) * 2 + core) * share, share)

    b_copies = {}
    for index, (s, t, g) in enumerate(items):
        if s == 0:
            continue
        at = ((s - 1) * nb + t) * SUBS + g
        send_b[at] = pair_sum(index, s, t, g).astype(BF16)
        copy = pltpu.make_async_remote_copy(
            src_ref=send_b.at[at],
            dst_ref=recv_b.at[at],
            send_sem=b_s.at[at],
            recv_sem=b_r.at[at],
            device_id={"dp": dp_of(lax.rem(a + s, na), b)},
            device_id_type=MESH,
        )
        copy.start()
        b_copies[s, t, g] = copy
    c_copies = {}
    for index, (s, t, g) in enumerate(items):
        if s > 0:
            continue
        total = pair_sum(index, s, t, g)
        for s_from in range(1, na):
            b_copies[s_from, t, g].wait_recv()
            total = total + recv_b[((s_from - 1) * nb + t) * SUBS + g].astype(F32)
        if t > 0:
            at = (t - 1) * SUBS + g
            send_c[at] = total.astype(BF16)
            copy = pltpu.make_async_remote_copy(
                src_ref=send_c.at[at],
                dst_ref=recv_c.at[at],
                send_sem=c_s.at[at],
                recv_sem=c_r.at[at],
                device_id={"dp": dp_of(a, lax.rem(b + t, nb))},
                device_id_type=MESH,
            )
            copy.start()
            c_copies[t, g] = copy
        else:
            w_grad_ref[0, pl.ds(g * sub, sub)] = total
    for t in range(1, nb):
        for g in range(SUBS):
            c_copies[t, g].wait_recv()
            w_grad_ref[0, pl.ds(g * sub, sub)] += recv_c[(t - 1) * SUBS + g].astype(F32)

    for k in near + far:
        returns[k].wait_recv()
    in_grad_ref[...] = jnp.dot(table_t, arrived[...], preferred_element_type=F32).astype(BF16)

    for k in near + far:
        x_copies[k].wait_send()
        g_copies[k].wait_send()
        returns[k].wait_send()
    for copy in a_copies + list(b_copies.values()) + list(c_copies.values()):
        copy.wait_send()


def local(n_expert, n_dp, tokens, out_grad, gate_prob, routing, expert_weights):
    tok, width = tokens.shape
    full = expert_weights.shape[2]
    hid = full // 3
    cap = max(16, 2 * tok // n_expert)
    slots = n_expert * cap
    share = width // n_dp
    _, _, _, na, nb = plan(n_expert, n_dp)
    sub = share // SUBS
    chips = na * nb
    n_b, n_c = max(1, (na - 1) * nb) * SUBS, max(1, nb - 1) * SUBS
    dma = pltpu.SemaphoreType.DMA
    vmem = pl.BlockSpec(memory_space=pltpu.VMEM)
    return pl.pallas_call(
        functools.partial(body, n_expert, n_dp, cap),
        out_shape=(
            jax.ShapeDtypeStruct((tok, width), BF16),
            jax.ShapeDtypeStruct((1, share, full), F32),
        ),
        in_specs=[vmem] * 5 + [pl.BlockSpec(memory_space=pl.ANY)],
        out_specs=(vmem, vmem),
        scratch_shapes=[
            pltpu.VMEM((width, full), BF16),
            pltpu.VMEM((slots, width), BF16),
            pltpu.VMEM((slots, width), BF16),
            pltpu.VMEM((slots, width), BF16),
            pltpu.VMEM((slots, width), BF16),
            pltpu.VMEM((slots, width), BF16),
            pltpu.VMEM((slots, width), BF16),
            pltpu.VMEM((slots, 2 * hid), BF16),
            pltpu.VMEM((slots, hid), BF16),
            pltpu.VMEM((width, full), BF16),
            pltpu.VMEM((chips * share, full), BF16),
            pltpu.VMEM((n_b, sub, full), BF16),
            pltpu.VMEM((n_b, sub, full), BF16),
            pltpu.VMEM((n_c, sub, full), BF16),
            pltpu.VMEM((n_c, sub, full), BF16),
            dma,
            dma((n_expert,)),
            dma((n_expert,)),
            dma((n_expert,)),
            dma((n_expert,)),
            dma((n_expert,)),
            dma((n_expert,)),
            dma((chips * SUBS,)),
            dma((chips * SUBS,)),
            dma((n_b,)),
            dma((n_b,)),
            dma((n_c,)),
            dma((n_c,)),
        ],
        compiler_params=pltpu.CompilerParams(
            collective_id=0, has_side_effects=True, vmem_limit_bytes=60 * 1024 * 1024
        ),
        name="moe_backward",
    )(tokens, out_grad, gate_prob, routing, routing.reshape(1, tok), expert_weights)


def solution(mesh):
    tokens_spec = P(("dp", "expert"), None)
    return jax.shard_map(
        functools.partial(local, mesh.shape["expert"], mesh.shape["dp"]),
        mesh=mesh,
        in_specs=(tokens_spec, tokens_spec, tokens_spec, tokens_spec, P("expert", None, None)),
        out_specs=(tokens_spec, P("expert", "dp", None)),
        check_vma=False,
    )
```

```python
import functools
import math
import jax
import jax.numpy as jnp
from jax import lax
from jax.experimental import pallas as pl
from jax.experimental.pallas import tpu as pltpu
from jax.sharding import PartitionSpec as P

MESH = pl.DeviceIdType.MESH
F32 = jnp.float32
BF16 = jnp.bfloat16
SUBS = 2
PIECES = 4


def xor(value, step):
    total, bit = 0, 1
    result = value
    while bit <= step:
        if step & bit:
            result = result + bit - 2 * bit * (lax.rem(lax.div(value, bit), 2))
        bit *= 2
    return result


def plan(n_expert, n_dp):
    half, quarter = n_expert // 2, n_expert // 4
    near = list(range(1, half))
    across = list(range(n_expert - 1, half + quarter - 1, -1))
    last = list(range(half + quarter - 1, half - 1, -1))
    chips = n_dp // 2
    side = math.isqrt(chips)
    while chips % side:
        side -= 1
    return near, across, last, chips // side, side


def body(
    n_expert,
    n_dp,
    cap,
    tokens_ref,
    out_grad_ref,
    gate_ref,
    route_ref,
    w_hbm,
    in_grad_ref,
    w_grad_ref,
    w_ref,
    send_x,
    send_g,
    recv_x,
    recv_g,
    ret,
    arrived,
    pair,
    hidden,
    part,
    recv_a,
    send_b,
    recv_b,
    send_c,
    recv_c,
    w_sem,
    dx_s,
    dx_r,
    dg_s,
    dg_r,
    rt_s,
    rt_r,
    a_s,
    a_r,
    b_s,
    b_r,
    c_s,
    c_r,
):
    near, across, last, na, nb = plan(n_expert, n_dp)
    far = across + last
    me = lax.axis_index("expert")
    dp = lax.axis_index("dp")
    tok, width = tokens_ref.shape
    hid = w_ref.shape[1] // 3
    slots = n_expert * cap
    quarter_rows = slots // 4
    share = width // n_dp
    sub = share // SUBS
    grad_scale = float(tok * n_dp) ** (-0.5)
    core = lax.rem(dp, 2)
    chip = lax.div(dp, 2)
    pos_hi, pos_lo = lax.div(chip, na), lax.rem(chip, na)
    if na == nb:
        a = jnp.where(core == 0, pos_lo, pos_hi)
        b = jnp.where(core == 0, pos_hi, pos_lo)
    else:
        a, b = pos_lo, pos_hi

    def chip_of(a_at, b_at):
        plain = b_at * na + a_at
        if na == nb:
            return jnp.where(core == 0, plain, a_at * na + b_at)
        return plain

    def dp_of(a_at, b_at):
        return chip_of(a_at, b_at) * 2 + core

    w_copy = pltpu.make_async_copy(w_hbm.at[0], w_ref, w_sem)
    w_copy.start()

    barrier = pltpu.get_barrier_semaphore()
    partner = dp + 1 - 2 * core
    greeted = 0
    for k in near + far:
        pl.semaphore_signal(barrier, inc=1, device_id={"expert": xor(me, k)}, device_id_type=MESH)
        greeted += 1
    pl.semaphore_signal(barrier, inc=1, device_id={"dp": partner}, device_id_type=MESH)
    greeted += 1
    for s in range(1, na):
        pl.semaphore_signal(
            barrier, inc=1, device_id={"dp": dp_of(lax.rem(a + s, na), b)}, device_id_type=MESH
        )
        greeted += 1
    for t in range(1, nb):
        pl.semaphore_signal(
            barrier, inc=1, device_id={"dp": dp_of(a, lax.rem(b + t, nb))}, device_id_type=MESH
        )
        greeted += 1

    row_i = lax.broadcasted_iota(jnp.int32, (tok, tok), 0)
    col_i = lax.broadcasted_iota(jnp.int32, (tok, tok), 1)

    def column(row):
        return jnp.sum(jnp.where(row_i == col_i, row, 0.0), axis=1, keepdims=True)

    route_row = route_ref[...].astype(F32)
    route_col = column(route_row)
    same = route_col == route_row
    pos_row = jnp.sum(jnp.where(same & (row_i < col_i), 1.0, 0.0), axis=0, keepdims=True)
    pos_col = jnp.sum(jnp.where(same & (col_i < row_i), 1.0, 0.0), axis=1, keepdims=True)
    slot_row = route_row * cap + pos_row
    slot_col = route_col * cap + pos_col
    slot_at = lax.broadcasted_iota(jnp.int32, (slots, tok), 0).astype(F32)
    table = jnp.where(slot_at == slot_row, 1.0, 0.0).astype(BF16)
    slot_of = lax.broadcasted_iota(jnp.int32, (tok, slots), 1).astype(F32)
    table_t = jnp.where(slot_of == slot_col, 1.0, 0.0).astype(BF16)

    send_x[...] = jnp.dot(table, tokens_ref[...], preferred_element_type=F32).astype(BF16)
    scaled = (column(gate_ref[...]) * out_grad_ref[...].astype(F32)).astype(BF16)
    send_g[...] = jnp.dot(table, scaled, preferred_element_type=F32).astype(BF16)

    def rows_of(index):
        return pl.ds(pl.multiple_of(index * cap, cap), cap)

    pl.semaphore_wait(barrier, greeted)

    def dispatch(k, src, dst, s_sem, r_sem):
        peer = xor(me, k)
        return pltpu.make_async_remote_copy(
            src_ref=src.at[rows_of(peer)],
            dst_ref=dst.at[rows_of(me)],
            send_sem=s_sem.at[k],
            recv_sem=r_sem.at[k],
            device_id={"expert": peer},
            device_id_type=MESH,
        )

    x_copies = {k: dispatch(k, send_x, recv_x, dx_s, dx_r) for k in near + far}
    g_copies = {k: dispatch(k, send_g, recv_g, dg_s, dg_r) for k in near + far}
    returns = {k: dispatch(k, ret, arrived, rt_s, rt_r) for k in near + far}
    for k in near + far:
        x_copies[k].start()
        g_copies[k].start()

    recv_x[rows_of(me)] = send_x[rows_of(me)]
    recv_g[rows_of(me)] = send_g[rows_of(me)]
    w_copy.wait()

    mine = lax.div(me, n_expert // 4)

    def forward(start, size):
        rows = pl.ds(pl.multiple_of(start, cap), size)
        x = recv_x[rows]
        pre_gate = jnp.dot(x, w_ref[:, :hid], preferred_element_type=F32)
        pre_up = jnp.dot(x, w_ref[:, hid : 2 * hid], preferred_element_type=F32)
        grad_hidden = jnp.dot(recv_g[rows], w_ref[:, 2 * hid :], preferred_element_type=F32)
        sig = jax.nn.sigmoid(pre_gate)
        active = pre_gate * sig
        hidden[rows] = (active * pre_up).astype(BF16)
        grad_gate = grad_hidden * pre_up * (sig * (1.0 + pre_gate * (1.0 - sig)))
        pair[rows, :hid] = grad_gate.astype(BF16)
        pair[rows, hid:] = (grad_hidden * active).astype(BF16)

    def backward(start, size):
        rows = pl.ds(pl.multiple_of(start, cap), size)
        tile = min(512, width)

        @pl.loop(0, width // tile)
        def _(j):
            at = pl.ds(pl.multiple_of(j * tile, tile), tile)
            ret[rows, at] = lax.dot_general(
                pair[rows],
                w_ref[at, : 2 * hid],
                (((1,), (1,)), ((), ())),
                preferred_element_type=F32,
            ).astype(BF16)

    near_half = (lax.div(mine, 2) * 2 * quarter_rows, 2 * quarter_rows)
    across_quarter = (xor(mine, 3) * quarter_rows, quarter_rows)
    last_quarter = (xor(mine, 2) * quarter_rows, quarter_rows)
    for k in near:
        x_copies[k].wait_recv()
        g_copies[k].wait_recv()
    forward(*near_half)
    backward(*near_half)
    for k in near:
        returns[k].start()
    arrived[rows_of(me)] = ret[rows_of(me)]
    for k in across:
        x_copies[k].wait_recv()
        g_copies[k].wait_recv()
    forward(*across_quarter)
    backward(*across_quarter)
    for k in last:
        x_copies[k].wait_recv()
        g_copies[k].wait_recv()
    for k in across:
        returns[k].start()
    forward(*last_quarter)

    def weight_rows(start, size):
        at = pl.ds(pl.multiple_of(start, size), size)
        contract = (((0,), (0,)), ((), ()))
        part[at, : 2 * hid] = (
            grad_scale
            * lax.dot_general(recv_x[:, at], pair[...], contract, preferred_element_type=F32)
        ).astype(BF16)
        part[at, 2 * hid :] = (
            grad_scale
            * lax.dot_general(recv_g[:, at], hidden[...], contract, preferred_element_type=F32)
        ).astype(BF16)

    def band(chip_at, core_at, g):
        return pl.ds(pl.multiple_of((chip_at * 2 + core_at) * share + g * sub, sub), sub)

    bands = [(s, t) for s in range(1, na) for t in list(range(1, nb)) + [0]]
    bands += [(0, t) for t in list(range(1, nb)) + [0]]
    items = [(s, t, g) for s, t in bands for g in range(SUBS)]

    def item_chip(s, t):
        return chip_of(lax.rem(a + s, na), lax.rem(b + t, nb))

    banded = share % 128 == 0
    if not banded:

        @pl.loop(0, width // 256)
        def _(j):
            weight_rows(j * 256, 256)

    def pair_copy(index, chip_at, g):
        rows = band(chip_at, 1 - core, g)
        return pltpu.make_async_remote_copy(
            src_ref=part.at[rows],
            dst_ref=recv_a.at[pl.ds(pl.multiple_of(chip_at * share + g * sub, sub), sub)],
            send_sem=a_s.at[index],
            recv_sem=a_r.at[index],
            device_id={"dp": partner},
            device_id_type=MESH,
        )

    def partner_chip(s, t):
        if na == nb:
            a_at, b_at = lax.rem(b + s, na), lax.rem(a + t, nb)
            return jnp.where(core == 1, b_at * na + a_at, a_at * na + b_at)
        return item_chip(s, t)

    a_copies = []
    for index, (s, t, g) in enumerate(items):
        chip_at = partner_chip(s, t)
        if banded and g == 0:
            weight_rows((chip_at * 2 + 1 - core) * share, share)
        copy = pair_copy(index, chip_at, g)
        copy.start()
        a_copies.append(copy)

    backward(*last_quarter)
    for k in last:
        returns[k].start()

    def pair_sum(index, s, t, g):
        chip_at = item_chip(s, t)
        a_copies[index].wait_recv()
        return (
            part[band(chip_at, core, g)].astype(F32)
            + recv_a[pl.ds(pl.multiple_of(chip_at * share + g * sub, sub), sub)].astype(F32)
        )

    if banded:
        for s, t in bands:
            weight_rows((item_chip(s, t) * 2 + core) * share, share)

    b_copies = {}
    for index, (s, t, g) in enumerate(items):
        if s == 0:
            continue
        at = ((s - 1) * nb + t) * SUBS + g
        send_b[at] = pair_sum(index, s, t, g).astype(BF16)
        copy = pltpu.make_async_remote_copy(
            src_ref=send_b.at[at],
            dst_ref=recv_b.at[at],
            send_sem=b_s.at[at],
            recv_sem=b_r.at[at],
            device_id={"dp": dp_of(lax.rem(a + s, na), b)},
            device_id_type=MESH,
        )
        copy.start()
        b_copies[s, t, g] = copy
    c_copies = {}
    for index, (s, t, g) in enumerate(items):
        if s > 0:
            continue
        total = pair_sum(index, s, t, g)
        for s_from in range(1, na):
            b_copies[s_from, t, g].wait_recv()
            total = total + recv_b[((s_from - 1) * nb + t) * SUBS + g].astype(F32)
        if t > 0:
            at = (t - 1) * SUBS + g
            send_c[at] = total.astype(BF16)
            copy = pltpu.make_async_remote_copy(
                src_ref=send_c.at[at],
                dst_ref=recv_c.at[at],
                send_sem=c_s.at[at],
                recv_sem=c_r.at[at],
                device_id={"dp": dp_of(a, lax.rem(b + t, nb))},
                device_id_type=MESH,
            )
            copy.start()
            c_copies[t, g] = copy
        else:
            w_grad_ref[0, pl.ds(g * sub, sub)] = total
    for t in range(1, nb):
        for g in range(SUBS):
            c_copies[t, g].wait_recv()
            w_grad_ref[0, pl.ds(g * sub, sub)] += recv_c[(t - 1) * SUBS + g].astype(F32)

    for k in near + far:
        returns[k].wait_recv()
    in_grad_ref[...] = jnp.dot(table_t, arrived[...], preferred_element_type=F32).astype(BF16)

    for k in near + far:
        x_copies[k].wait_send()
        g_copies[k].wait_send()
        returns[k].wait_send()
    for copy in a_copies + list(b_copies.values()) + list(c_copies.values()):
        copy.wait_send()


def local(n_expert, n_dp, tokens, out_grad, gate_prob, routing, expert_weights):
    tok, width = tokens.shape
    full = expert_weights.shape[2]
    hid = full // 3
    cap = max(16, 2 * tok // n_expert)
    slots = n_expert * cap
    share = width // n_dp
    _, _, _, na, nb = plan(n_expert, n_dp)
    sub = share // SUBS
    chips = na * nb
    n_b, n_c = max(1, (na - 1) * nb) * SUBS, max(1, nb - 1) * SUBS
    dma = pltpu.SemaphoreType.DMA
    vmem = pl.BlockSpec(memory_space=pltpu.VMEM)
    early = pl.pallas_call(
        functools.partial(body, n_expert, n_dp, cap),
        out_shape=(
            jax.ShapeDtypeStruct((tok, width), BF16),
            jax.ShapeDtypeStruct((1, share, full), F32),
        ),
        in_specs=[vmem] * 4 + [pl.BlockSpec(memory_space=pl.ANY)],
        out_specs=(vmem, vmem),
        scratch_shapes=[
            pltpu.VMEM((width, full), BF16),
            pltpu.VMEM((slots, width), BF16),
            pltpu.VMEM((slots, width), BF16),
            pltpu.VMEM((slots, width), BF16),
            pltpu.VMEM((slots, width), BF16),
            pltpu.VMEM((slots, width), BF16),
            pltpu.VMEM((slots, width), BF16),
            pltpu.VMEM((slots, 2 * hid), BF16),
            pltpu.VMEM((slots, hid), BF16),
            pltpu.VMEM((width, full), BF16),
            pltpu.VMEM((chips * share, full), BF16),
            pltpu.VMEM((n_b, sub, full), BF16),
            pltpu.VMEM((n_b, sub, full), BF16),
            pltpu.VMEM((n_c, sub, full), BF16),
            pltpu.VMEM((n_c, sub, full), BF16),
            dma,
            dma((n_expert,)),
            dma((n_expert,)),
            dma((n_expert,)),
            dma((n_expert,)),
            dma((n_expert,)),
            dma((n_expert,)),
            dma((chips * SUBS,)),
            dma((chips * SUBS,)),
            dma((n_b,)),
            dma((n_b,)),
            dma((n_c,)),
            dma((n_c,)),
        ],
        compiler_params=pltpu.CompilerParams(
            collective_id=0, has_side_effects=True, vmem_limit_bytes=60 * 1024 * 1024
        ),
        name="moe_backward",
    )(tokens, out_grad, gate_prob.reshape(1, tok), routing.reshape(1, tok), expert_weights)
    return pl.pallas_call(
        write_out,
        out_shape=(
            jax.ShapeDtypeStruct((tok, width), BF16),
            jax.ShapeDtypeStruct((1, share, full), F32),
        ),
        in_specs=[pl.BlockSpec(memory_space=pl.ANY)] * 2,
        out_specs=(pl.BlockSpec(memory_space=pl.ANY),) * 2,
        scratch_shapes=[
            pltpu.VMEM((tok, width), BF16),
            pltpu.VMEM((1, share, full), F32),
            dma((2 * PIECES,)),
            dma((2 * PIECES,)),
        ],
        name="write_out",
    )(*early)


def write_out(in_grad_ref, w_grad_ref, in_grad_out, w_grad_out, x_held, w_held, in_s, out_s):
    moves = []
    for p in range(PIECES):
        for src, mid, dst in (
            (in_grad_ref, x_held, in_grad_out),
            (w_grad_ref.at[0], w_held.at[0], w_grad_out.at[0]),
        ):
            rows = src.shape[0] // PIECES
            at = pl.ds(p * rows, rows)
            n = len(moves)
            moves.append(
                (
                    pltpu.make_async_copy(src.at[at], mid.at[at], in_s.at[n]),
                    pltpu.make_async_copy(mid.at[at], dst.at[at], out_s.at[n]),
                )
            )
    for take, _ in moves:
        take.start()
    for take, put in moves:
        take.wait()
        put.start()
    for _, put in moves:
        put.wait()


def solution(mesh):
    tokens_spec = P(("dp", "expert"), None)
    return jax.shard_map(
        functools.partial(local, mesh.shape["expert"], mesh.shape["dp"]),
        mesh=mesh,
        in_specs=(tokens_spec, tokens_spec, tokens_spec, tokens_spec, P("expert", None, None)),
        out_specs=(tokens_spec, P("expert", "dp", None)),
        check_vma=False,
    )
```
